32 devices in a mesh: seq: 8 (over z, core), exp: 4 (over y, x).
Axes of the slice: x: 2, y: 2, z: 4, core: 2. Of those that a mesh axis runs over, the one named last changes fastest.
Arguments:
- queries: bfloat16 [768, 4096], P('seq', 'exp'), may hold values from -17 to 17
- keys: bfloat16 [768, 1024], P('seq', 'exp'), may hold values from -17 to 17
- values: bfloat16 [768, 1024], P('seq', 'exp'), may hold values from -6 to 6
- residual: bfloat16 [768, 4096], P('seq', 'exp'), may hold values from -48 to 48
- norm_gain: float32 [4096], P('exp'), may hold values from 0.1 to 1.9
- routes: int32 [768, 2], P('seq'), may hold values from 0 to 3, all different within a row; in each aligned block of 96 rows (0 to 95, 96 to 191, ...) at most 72 rows name the same one
- gates: float32 [768, 2], P('seq'), may hold values from 0.1 to 0.9
- w_gate: bfloat16 [4, 4096, 14336], P('exp', None, 'seq'), may hold values from -0.09375 to 0.09375
- w_up: bfloat16 [4, 4096, 14336], P('exp', None, 'seq'), may hold values from -0.09375 to 0.09375
- w_down: bfloat16 [4, 14336, 4096], P('exp', 'seq'), may hold values from -0.046875 to 0.046875
Outputs:
- attended: bfloat16 [768, 4096], P('seq', 'exp')
- layer_out: bfloat16 [768, 4096], P('seq', 'exp')
The draws below stay inside these ranges and needn't reach their ends.
Inputs may be any that keep to these rules, and one draw needn't show every extreme that they name: `routes`: each row names 2 different experts. In the rows of one device no expert is named more than 72 times, a bound that some block reaches.
All inputs are finite; a program needn't handle non-finite values.
Results may differ from the reference program's by a relative error of at most 0.0075.
Values may be sent and summed in bfloat16 or wider, within the bound.
A program may use at most 128 MiB of HBM per device.

```python
import math
import jax
import jax.numpy as jnp
import numpy as np
from jax import lax

D = 4096
QUERY_HEADS = 32
KEY_VALUE_HEADS = 8
HEAD_WIDTH = 128
FF = 14336
TOP = 2
TOK_DEV = 96
SEQUENCE_LENGTH = 768
EXPERTS = 4
CAP = 72
N_SEQ = 8


def draw_keys(key, part):
    layer_result = jnp.clip(jax.random.normal(jax.random.fold_in(key, 2), (SEQUENCE_LENGTH, KEY_VALUE_HEADS * HEAD_WIDTH), jnp.float32), -4.0, 4.0)
    layer_result = jnp.clip(layer_result, -16.5, 16.5)
    return layer_result.astype(jnp.bfloat16)


def draw_queries(key, part):
    layer_result = jnp.clip(jax.random.normal(jax.random.fold_in(key, 1), (SEQUENCE_LENGTH, QUERY_HEADS * HEAD_WIDTH), jnp.float32), -4.0, 4.0)
    layer_result = jnp.clip(layer_result, -16.5, 16.5)
    return layer_result.astype(jnp.bfloat16)


def draw_residual(key, part):
    base = jnp.clip(jax.random.normal(jax.random.fold_in(key, 5), (SEQUENCE_LENGTH, D), jnp.float32), -4.0, 4.0)
    column = jnp.arange(D, dtype=jnp.float32) / max(D - 1, 1)
    column_scale = 0.6 * jnp.exp(column * math.log(5.0))
    layer_result = base * column_scale[None, :]
    return layer_result.astype(jnp.bfloat16)


def steps_of(key, extent, shards, smallest, top_value):
    loudness = 1.0
    for axis_at, shards_of in shards:
        steps = jax.random.uniform(jax.random.fold_in(jax.random.fold_in(key, 6), axis_at), (shards_of,), jnp.float32, smallest / len(shards), top_value / len(shards))
        loudness = loudness * jnp.repeat(jnp.exp(steps), extent[axis_at] // shards_of).reshape((-1,) + (1,) * (len(extent) - 1 - axis_at))
    return loudness


def assign_block(key, own, number, rows, amount, top, bound, skew):
    ranking = jax.random.permutation(key, amount)
    packed, common = shares(amount, rows * top, bound, skew, True), shares(amount, rows * top, bound, skew, False)
    places = jnp.arange(amount)

    def named(tallies, offset_by):
        used = int((tallies > 0).sum())
        fixed = max(1, used // 4)
        moved = fixed + (places - fixed + offset_by * (used - fixed)) % max(1, amount - fixed)
        return jnp.zeros((amount,), jnp.int32).at[ranking[jnp.where(places < fixed, places, moved)]].set(jnp.asarray(tallies, jnp.int32))

    tallies = jnp.where(number % 4 == 0, named(packed, number // 4), named(common, number - number // 4 - 1))
    mixed = jax.random.permutation(jax.random.fold_in(own, 3), amount)
    source_of, taker = mixed[0:amount // 2 * 2:2], mixed[1:amount // 2 * 2:2]
    room = jnp.minimum(tallies[source_of] - 1, bound - tallies[taker]) // 2
    room = jnp.where((source_of == ranking[0]) | (taker == ranking[0]) | (tallies[taker] == 0), 0, jnp.maximum(room, 0))
    moved = jax.random.randint(jax.random.fold_in(own, 4), (amount // 2,), 0, 1 << 20) % (room + 1)
    tallies = tallies.at[source_of].add(-moved).at[taker].add(moved)
    labels = jnp.searchsorted(jnp.cumsum(tallies), jnp.arange(rows * top), side="right").astype(jnp.int32)
    grid = labels.reshape(top, rows).T
    grid = grid[jax.random.permutation(jax.random.fold_in(own, 1), rows)]
    offset_by = jax.random.randint(jax.random.fold_in(own, 2), (rows, 1), 0, top)
    return jnp.take_along_axis(grid, (jnp.arange(top)[None, :] + offset_by) % top, axis=1)


def shares(number_of, total, limit, lean, full):
    loads = [(1 << 20) // math.isqrt(rank ** lean) + 1 for rank in range(1, number_of + 1)]
    largest = limit if full else min(limit, max(-(-total // number_of), total * loads[0] // sum(loads)))
    least = 1 if total - largest >= number_of - 1 else 0
    given, rest = [largest] + [least] * (number_of - 1), total - largest - least * (number_of - 1)
    while rest > 0:
        free = [i for i in range(1, number_of) if given[i] < largest] or [i for i in range(1, number_of) if given[i] < limit]
        pool, left = sum([loads[i] for i in free]), rest
        for i in free:
            more = min(limit - given[i], max(1, left * loads[i] // pool), rest)
            given[i] = given[i] + more
            rest = rest - more
    return np.array(given)


def noise(stream_key, extent, deviation, limit, split=(), kind=jnp.bfloat16):
    result = deviation * jax.random.normal(stream_key, extent, jnp.float32)
    if split:
        result = result * steps_of(stream_key, extent, split, -0.22, 0.18)
    return jnp.clip(result, -limit, limit).astype(kind)


def setup_inputs(seed: int = 0) -> dict:
    seeds = jax.random.split(jax.random.key(seed), 11)
    queries = draw_queries(jax.random.fold_in(seeds[10], 71), 0)
    keys = draw_keys(jax.random.fold_in(seeds[10], 71), 0)
    values = noise(seeds[2], (SEQUENCE_LENGTH, KEY_VALUE_HEADS * HEAD_WIDTH), 1.0, 6.0, ((0, 8), (1, 4)))
    residual = draw_residual(jax.random.fold_in(seeds[10], 71), 0)
    norm_gain = jnp.clip(1.0 + 0.18 * jax.random.normal(seeds[4], (D,), jnp.float32), 0.1, 1.9)
    routes_keys = jax.random.split(jax.random.fold_in(seeds[5], 1), SEQUENCE_LENGTH // TOK_DEV)
    routes_turns = jax.random.permutation(jax.random.fold_in(seeds[5], 3), SEQUENCE_LENGTH // TOK_DEV)
    routes = jax.vmap(lambda own, number: assign_block(jax.random.fold_in(seeds[5], 2), own, number, TOK_DEV, EXPERTS, TOP, CAP, 2))(routes_keys, routes_turns).reshape((SEQUENCE_LENGTH, TOP))
    gates = jnp.clip(0.1 + 0.79999997 * jax.random.uniform(seeds[6], (SEQUENCE_LENGTH, TOP), jnp.float32) ** steps_of(seeds[6], (SEQUENCE_LENGTH, TOP), ((0, 8),), -0.2, 0.2), 0.1, 0.9)
    w_gate = noise(seeds[7], (EXPERTS, D, FF), D ** -0.5, 0.09375, ((0, 4), (2, 8)))
    w_up = noise(seeds[8], (EXPERTS, D, FF), D ** -0.5, 0.09375, ((0, 4), (2, 8)))
    w_down = noise(seeds[9], (EXPERTS, FF, D), FF ** -0.5, 0.046875, ((0, 4), (1, 8)))
    return {"queries": queries, "keys": keys, "values": values, "residual": residual, "norm_gain": norm_gain, "routes": routes, "gates": gates, "w_gate": w_gate, "w_up": w_up, "w_down": w_down}


def attend_head(inputs):
    query_head, key_head, value_head = inputs
    scores = jnp.einsum('tgd,pd->gtp', query_head, key_head) / math.sqrt(HEAD_WIDTH)
    positions = jnp.arange(SEQUENCE_LENGTH, dtype=jnp.int32)
    causal_mask = (positions[None, :] <= positions[:, None])[None, :, :]
    scores = jnp.where(causal_mask, scores, -1e+30)
    row_max = lax.optimization_barrier(jnp.max(scores, axis=-1, keepdims=True))
    exp_terms = jnp.where(causal_mask, jnp.exp(scores - row_max), 0.0)
    denominator = lax.optimization_barrier(jnp.sum(exp_terms, axis=-1))
    probs_low = exp_terms.astype(jnp.bfloat16).astype(jnp.float32)
    return jnp.einsum('gtp,pd->gtd', probs_low, value_head) / denominator[..., None]

def expert_apply(inputs):
    rows, gate_mat, up_mat, down_mat = inputs
    hidden = (jax.nn.silu(jnp.dot(rows, gate_mat, preferred_element_type=jnp.float32)) * jnp.dot(rows, up_mat, preferred_element_type=jnp.float32)).astype(jnp.bfloat16)
    row_count = rows.shape[0]
    block_width = FF // N_SEQ
    hidden_blocks = jnp.transpose(hidden.reshape(row_count, N_SEQ, block_width), (1, 0, 2))
    down_blocks = down_mat.reshape(N_SEQ, block_width, D)

    def add_block(total, pair):
        hidden_block, down_block = pair
        term = jnp.dot(hidden_block, down_block, preferred_element_type=jnp.float32).astype(jnp.bfloat16)
        term = lax.optimization_barrier(term)
        return (total + term.astype(jnp.float32), None)
    total, unused = lax.scan(add_block, jnp.zeros((row_count, D), jnp.float32), (hidden_blocks, down_blocks))
    return total.astype(jnp.bfloat16)

def reference(queries, keys, values, residual, norm_gain, routes, gates, w_gate, w_up, w_down):
    group_width = QUERY_HEADS // KEY_VALUE_HEADS
    query_head_rows = jnp.transpose(queries.astype(jnp.float32).reshape(SEQUENCE_LENGTH, KEY_VALUE_HEADS, group_width, HEAD_WIDTH), (1, 0, 2, 3))
    key_head_rows = jnp.transpose(keys.astype(jnp.float32).reshape(SEQUENCE_LENGTH, KEY_VALUE_HEADS, HEAD_WIDTH), (1, 0, 2))
    value_head_rows = jnp.transpose(values.astype(jnp.float32).reshape(SEQUENCE_LENGTH, KEY_VALUE_HEADS, HEAD_WIDTH), (1, 0, 2))
    heads_out = lax.map(attend_head, (query_head_rows, key_head_rows, value_head_rows))
    attn = jnp.transpose(heads_out, (2, 0, 1, 3)).reshape(SEQUENCE_LENGTH, QUERY_HEADS * HEAD_WIDTH)
    attended = (residual.astype(jnp.float32) + attn).astype(jnp.bfloat16)
    stream = attended.astype(jnp.float32)
    mean_square = lax.optimization_barrier(jnp.mean(stream * stream, axis=-1, keepdims=True))
    inverse_root = lax.rsqrt(mean_square + 1e-05)
    normed = (stream * inverse_root * norm_gain.astype(jnp.float32)).astype(jnp.bfloat16)
    blocks = N_SEQ
    assigned = TOK_DEV * TOP
    normed_blocks = normed.reshape(blocks, TOK_DEV, D)
    route_blocks = routes.reshape(blocks, assigned).astype(jnp.int32)
    one_hot = (route_blocks[:, :, None] == jnp.arange(EXPERTS, dtype=jnp.int32)[None, None, :]).astype(jnp.int32)
    before = jnp.cumsum(one_hot, axis=1) - one_hot
    slot_index = lax.optimization_barrier(jnp.sum(before * one_hot, axis=-1)).astype(jnp.int32)
    dest_slot = (route_blocks * CAP + slot_index).astype(jnp.int32)
    selected = (dest_slot[:, :, None] == jnp.arange(EXPERTS * CAP, dtype=jnp.int32)[None, None, :]).astype(jnp.int32)
    token_of = (jnp.arange(assigned, dtype=jnp.int32) // TOP)[None, :, None]
    token_index = lax.optimization_barrier(jnp.sum(selected * token_of, axis=1)).astype(jnp.int32)
    filled = lax.optimization_barrier(jnp.sum(selected, axis=1))
    slot_rows = jnp.take_along_axis(normed_blocks, token_index[:, :, None], axis=1)
    slot_rows = jnp.where(filled[:, :, None] > 0, slot_rows, jnp.zeros_like(slot_rows))
    by_expert = jnp.transpose(slot_rows.reshape(blocks, EXPERTS, CAP, D), (1, 0, 2, 3)).reshape(EXPERTS, blocks * CAP, D)
    expert_out = lax.map(expert_apply, (by_expert, w_gate, w_up, w_down))
    flat_out = expert_out.reshape(EXPERTS * blocks * CAP, D)
    block_ids = jnp.arange(blocks, dtype=jnp.int32)[:, None]
    flat_index = ((route_blocks * blocks + block_ids) * CAP + slot_index).astype(jnp.int32)
    picked = flat_out[flat_index].astype(jnp.float32).reshape(blocks, TOK_DEV, TOP, D)
    gate_blocks = gates.astype(jnp.float32).reshape(blocks, TOK_DEV, TOP)
    mixture = lax.optimization_barrier(jnp.sum(gate_blocks[..., None] * picked, axis=2)).reshape(SEQUENCE_LENGTH, D)
    layer_out = (stream + mixture).astype(jnp.bfloat16)
    return (attended, layer_out)
```

```python
import functools
import math
import types

import jax
import jax.numpy as jnp
from jax import lax
from jax.experimental import pallas as pl
from jax.experimental.pallas import tpu as pltpu
from jax.sharding import PartitionSpec as P

D = 4096
QUERY_HEADS = 32
KEY_VALUE_HEADS = 8
HEAD_WIDTH = 128
TOP = 2
CORES = 2
LANES = 128
BF16 = jnp.bfloat16
F32 = jnp.float32


def place(chips, exp_count):
    seq, exp = lax.axis_index("seq"), lax.axis_index("exp")
    chip, core = seq // CORES, lax.rem(seq, CORES)
    far = lambda d: {"seq": lax.rem(chip + d, chips) * CORES + core, "exp": exp}
    partner = {"seq": chip * CORES + 1 - core, "exp": exp}
    side = lambda d: {"seq": seq, "exp": lax.rem(exp + d, exp_count)}
    return seq, exp, chip, core, far, partner, side


def greet(chips, exp_count, far, partner, side):
    barrier = pltpu.get_barrier_semaphore()
    targets = [partner]
    targets += [far(d) for d in range(1, chips)]
    targets += [side(d) for d in range(1, exp_count)]
    for target in targets:
        pl.semaphore_signal(barrier, inc=1, device_id=target, device_id_type=pl.DeviceIdType.MESH)
    pl.semaphore_wait(barrier, len(targets))


def remote(src, dst, send_sem, recv_sem, target):
    return pltpu.make_async_remote_copy(
        src_ref=src,
        dst_ref=dst,
        send_sem=send_sem,
        recv_sem=recv_sem,
        device_id=target,
        device_id_type=pl.DeviceIdType.MESH,
    )


def share_kernel(
    chips, exp_count, capacity, k_ref, v_ref, raw_ref, gain_ref,
    k_all, v_all, meta_all, gain_all,
    meta_ref, far_send, far_recv, fwd_send, fwd_recv, side_send, side_recv, local_sem,
):
    seq, exp, chip, core, far, partner, side = place(chips, exp_count)
    greet(chips, exp_count, far, partner, side)
    sent = []
    pairs = ((k_ref, k_all), (v_ref, v_all))
    for d in range(chips - 1, 0, -1):
        for i, (src, dst) in enumerate(pairs):
            c = remote(src, dst.at[seq], far_send.at[i, d], far_recv.at[i, d], far(d))
            c.start()
            sent.append(c)
    for d in range(1, exp_count):
        c = remote(gain_ref, gain_all.at[exp], side_send.at[d], side_recv.at[d], side(d))
        c.start()
        sent.append(c)
    for i, (src, dst) in enumerate(pairs):
        c = remote(src, dst.at[seq], fwd_send.at[i, 0], fwd_recv.at[i, 0], partner)
        c.start()
        sent.append(c)
    names = lax.broadcasted_iota(jnp.int32, raw_ref.shape, 0).astype(F32)
    one = [jnp.where(names == raw_ref[k : k + 1, :], 1.0, 0.0) for k in range(TOP)]
    lanes = (LANES, LANES)
    earlier = jnp.where(
        lax.broadcasted_iota(jnp.int32, lanes, 0) < lax.broadcasted_iota(jnp.int32, lanes, 1), 1.0, 0.0
    )
    before = jnp.dot(
        sum(one).astype(BF16), earlier.astype(BF16), preferred_element_type=F32
    )
    meta_ref[...] = raw_ref[...]
    for k in range(TOP):
        meta_ref[k : k + 1, :] = raw_ref[k : k + 1, :] * capacity + jnp.sum(
            one[k] * before, axis=0, keepdims=True
        )
    for d in range(chips - 1, 0, -1):
        c = remote(meta_ref, meta_all.at[chip], far_send.at[2, d], far_recv.at[2, d], far(d))
        c.start()
        sent.append(c)
    own = [
        pltpu.make_async_copy(src, dst, local_sem.at[i])
        for i, (src, dst) in enumerate(
            (
                (k_ref, k_all.at[seq]),
                (v_ref, v_all.at[seq]),
                (meta_ref, meta_all.at[chip]),
                (gain_ref, gain_all.at[exp]),
            )
        )
    ]
    for c in own:
        c.start()
    for d in range(1, chips):
        source = lax.rem(chip - d + chips, chips)
        block = source * CORES + core
        for i, (src, dst) in enumerate(pairs):
            remote(src, dst.at[block], far_send.at[i, d], far_recv.at[i, d], far(d)).wait_recv()
            c = remote(dst.at[block], dst.at[block], fwd_send.at[i, d], fwd_recv.at[i, d], partner)
            c.start()
            sent.append(c)
        remote(
            meta_ref, meta_all.at[source], far_send.at[2, d], far_recv.at[2, d], far(d)
        ).wait_recv()
    for d in range(1, exp_count):
        source = lax.rem(exp - d + exp_count, exp_count)
        remote(gain_ref, gain_all.at[source], side_send.at[d], side_recv.at[d], side(d)).wait_recv()
    for d in range(chips):
        block = lax.rem(chip - d + chips, chips) * CORES + 1 - core
        for i, (src, dst) in enumerate(pairs):
            remote(src, dst.at[block], fwd_send.at[i, d], fwd_recv.at[i, d], partner).wait_recv()
    for c in own:
        c.wait()
    for c in sent:
        c.wait_send()


def select_rows(dest, expert, member, capacity, iota):
    low = (expert * capacity).astype(F32)
    inside = (dest >= low) & (dest < low + capacity)
    return iota == jnp.where(inside, dest - low + (member * capacity).astype(F32), -1.0)


def gather_kernel(
    chips, exp_count, group, capacity, x_ref, meta_ref, gain_ref, gate_ref, up_ref, hidden_ref,
    out_ref, gate_mat, up_mat, tokens, outbox, inbox,
    far_send, far_recv, side_send, side_recv, pair_send, pair_recv, load_sem,
):
    seq, exp, chip, core, far, partner, side = place(chips, exp_count)
    blocks, depth, block = gate_mat.shape
    loads = []
    for i in range(blocks):
        for m, (src, dst) in enumerate(((gate_ref, gate_mat), (up_ref, up_mat))):
            c = pltpu.make_async_copy(
                src.at[:, i * block : (i + 1) * block], dst.at[i], load_sem.at[m, i]
            )
            c.start()
            loads.append(c)
    greet(chips, exp_count, far, partner, side)
    groups = chips // group
    tok_rows, width = x_ref.shape
    rows = group * capacity
    sent = []
    home, base = chip // group, lax.rem(chip, group)
    for slot in range(1, chips):
        turn, j = divmod(slot, group)
        target = lax.rem(home - turn + groups, groups) * group + lax.rem(base - j + group, group)
        c = remote(
            x_ref, tokens.at[slot], far_send.at[slot], far_recv.at[slot],
            {"seq": target * CORES + core, "exp": exp},
        )
        c.start()
        sent.append(c)
    tokens[0] = x_ref[...]
    iota = lax.broadcasted_iota(jnp.int32, (rows, tok_rows), 0).astype(F32)

    def dispatch(turn):
        which = lax.rem(home + turn, groups)
        members = []
        for j in range(group):
            place_of = lax.rem(base + j, group)
            slot = turn * group + j
            if slot:
                remote(
                    x_ref, tokens.at[slot], far_send.at[slot], far_recv.at[slot], partner
                ).wait_recv()
            members.append((which * group + place_of, place_of, slot))
        for step in range(exp_count):
            d = (step + 1) % exp_count
            expert = lax.rem(exp + d, exp_count)
            total = jnp.zeros((rows, width), F32)
            for source, member, slot in members:
                dest0 = meta_ref[source, 0:1, 0:tok_rows]
                dest1 = meta_ref[source, 1:2, 0:tok_rows]
                pick = select_rows(dest0, expert, member, capacity, iota) | select_rows(
                    dest1, expert, member, capacity, iota
                )
                total = total + jnp.dot(
                    jnp.where(pick, 1.0, 0.0).astype(BF16),
                    tokens[slot],
                    preferred_element_type=F32,
                )
            if d == 0:
                inbox[which, exp] = total.astype(BF16)
            else:
                outbox[turn, d - 1] = total.astype(BF16)
                c = remote(
                    outbox.at[turn, d - 1],
                    inbox.at[which, exp],
                    side_send.at[turn, d],
                    side_recv.at[turn, d],
                    side(d),
                )
                c.start()
                sent.append(c)

    def finish(turn):
        which = lax.rem(home + turn, groups)
        for d in range(1, exp_count):
            source = lax.rem(exp - d + exp_count, exp_count)
            remote(
                outbox.at[turn, d - 1],
                inbox.at[which, source],
                side_send.at[turn, d],
                side_recv.at[turn, d],
                side(d),
            ).wait_recv()
        step_rows = 16

        def norm(i, carry):
            at = pl.ds(pl.multiple_of(i * step_rows, step_rows), step_rows)
            square = jnp.zeros((step_rows, 1), F32)
            for e in range(exp_count):
                part = inbox[which, e, at, :].astype(F32)
                square = square + jnp.sum(part * part, axis=1, keepdims=True)
            scale = lax.rsqrt(square / (width * exp_count) + 1e-05)
            for e in range(exp_count):
                part = inbox[which, e, at, :].astype(F32)
                out_ref[which, core, at, e * width : (e + 1) * width] = (
                    part * scale * gain_ref[e, 0:1, :]
                ).astype(BF16)
            return carry

        lax.fori_loop(0, rows // step_rows, norm, 0)
        c = remote(
            out_ref.at[which, core],
            out_ref.at[which, core],
            pair_send.at[turn],
            pair_recv.at[turn],
            partner,
        )
        c.start()
        sent.append(c)

    for turn in range(groups):
        dispatch(turn)
    def expand(turn):
        which = lax.rem(home + turn, groups)
        remote(
            out_ref.at[which, core],
            out_ref.at[which, 1 - core],
            pair_send.at[turn],
            pair_recv.at[turn],
            partner,
        ).wait_recv()

        def one(i, carry):
            x = out_ref[which].reshape(CORES * rows, depth)
            gate = jnp.dot(x, gate_mat[i], preferred_element_type=F32)
            up = jnp.dot(x, up_mat[i], preferred_element_type=F32)
            hidden_ref[which, i] = (gate / (1.0 + jnp.exp(-gate)) * up).astype(BF16)
            return carry

        lax.fori_loop(0, blocks, one, 0)

    for c in loads:
        c.wait()
    for turn in range(groups):
        finish(turn)
        expand(turn)
    for c in sent:
        c.wait_send()


def return_kernel(
    chips, exp_count, group, capacity, hidden_ref, x_ref, meta_ref, down_ref, out_ref,
    down_mat, mine, peer, outbox, inbox, zout, zin,
    far_send, far_recv, side_send, side_recv, pair_send, pair_recv, load_sem,
):
    seq, exp, chip, core, far, partner, side = place(chips, exp_count)
    groups = chips // group
    tok_rows, width = x_ref.shape
    rows = group * capacity
    home = chip // group
    blocks, block = hidden_ref.shape[1], hidden_ref.shape[3]
    turns = [(step + 1) % exp_count for step in range(exp_count)]
    loads = {}
    for d in turns:
        columns = pl.ds(pl.multiple_of(lax.rem(exp + d, exp_count) * width, width), width)
        loads[d] = pltpu.make_async_copy(down_ref.at[:, columns], down_mat.at[d], load_sem.at[d])
        loads[d].start()
    greet(chips, exp_count, far, partner, side)
    order = list(range(1, groups)) + [0]
    sent = []

    def which_of(turn):
        return lax.rem(home - turn + groups, groups)

    def pair(turn, d):
        return remote(
            mine.at[turn, d, 1 - core],
            peer.at[turn, d],
            pair_send.at[turn, d],
            pair_recv.at[turn, d],
            partner,
        )

    def project(turn, d):
        which = which_of(turn)
        total = jnp.zeros((CORES * rows, width), F32)
        for i in range(blocks):
            total = total + jnp.dot(
                hidden_ref[which, i],
                down_mat[d, i * block : (i + 1) * block, :],
                preferred_element_type=F32,
            )
        mine[turn, d] = total.astype(BF16).reshape(CORES, rows, width)
        c = pair(turn, d)
        c.start()
        sent.append(c)

    def forward(turn, d):
        pair(turn, d).wait_recv()
        both = (mine[turn, d, core].astype(F32) + peer[turn, d].astype(F32)).astype(BF16)
        if d == 0:
            inbox[which_of(turn), exp] = both
        else:
            outbox[turn, d - 1] = both
            c = remote(
                outbox.at[turn, d - 1],
                inbox.at[which_of(turn), exp],
                side_send.at[turn, d],
                side_recv.at[turn, d],
                side(d),
            )
            c.start()
            sent.append(c)

    last = None
    for turn in order:
        for d in turns:
            if turn == order[0]:
                loads[d].wait()
            project(turn, d)
            if last is not None:
                forward(*last)
            last = (turn, d)
    forward(*last)
    iota = lax.broadcasted_iota(jnp.int32, (tok_rows, rows), 1).astype(F32)

    def mix(source, which, member):
        picked = [jnp.zeros((tok_rows, width), F32) for _ in range(TOP)]
        for e in range(exp_count):
            block = inbox[which, e]
            for k in range(TOP):
                dest = meta_ref[source, :, k : k + 1]
                low = float(e * capacity)
                inside = (dest >= low) & (dest < low + capacity)
                pick = iota == jnp.where(inside, dest - low + member.astype(F32) * capacity, -1.0)
                picked[k] = picked[k] + jnp.dot(
                    jnp.where(pick, 1.0, 0.0).astype(BF16), block, preferred_element_type=F32
                )
        total = jnp.zeros((tok_rows, width), F32)
        for k in range(TOP):
            total = total + picked[k] * meta_ref[source, :, TOP + k : TOP + k + 1]
        return total

    def arrive(turn):
        which = which_of(turn)
        for d in range(1, exp_count):
            source = lax.rem(exp - d + exp_count, exp_count)
            remote(
                outbox.at[turn, d - 1],
                inbox.at[which, source],
                side_send.at[turn, d],
                side_recv.at[turn, d],
                side(d),
            ).wait_recv()

    base = lax.rem(chip, group)
    total = None
    for turn in order:
        which = which_of(turn)
        arrive(turn)
        for j in range(group - 1, -1, -1):
            member = lax.rem(base + group - j, group)
            target = which * group + member
            part = mix(target, which, member)
            if turn == 0 and j == 0:
                total = part
            else:
                slot = turn * group + j
                zout[slot] = part.astype(BF16)
                c = remote(
                    zout.at[slot],
                    zin.at[slot],
                    far_send.at[slot],
                    far_recv.at[slot],
                    {"seq": target * CORES + core, "exp": exp},
                )
                c.start()
                sent.append(c)
    total = total + x_ref[...].astype(F32)
    for slot in range(1, chips):
        remote(
            zout.at[slot], zin.at[slot], far_send.at[slot], far_recv.at[slot], partner
        ).wait_recv()
        total = total + zin[slot].astype(F32)
    out_ref[...] = total.astype(BF16)
    for c in sent:
        c.wait_send()


def call(kernel, outs, scratch, collective_id, *args, streamed=()):
    vmem = pl.BlockSpec(memory_space=pltpu.VMEM)
    any_space = pl.BlockSpec(memory_space=pl.ANY)
    return pl.pallas_call(
        kernel,
        out_shape=outs,
        in_specs=[vmem] * len(args) + [any_space] * len(streamed),
        out_specs=jax.tree.map(lambda _: vmem, outs),
        scratch_shapes=scratch,
        compiler_params=pltpu.CompilerParams(
            collective_id=collective_id, has_side_effects=True, vmem_limit_bytes=56 * 2**20
        ),
    )(*args, *streamed)


def flip(index, step):
    bit = 1
    while bit <= step:
        if step & bit:
            index = index + bit - 2 * bit * lax.rem(index // bit, 2)
        bit *= 2
    return index


RANKS = 4
PLAN = (
    "F0", "T1", "T2", "T3", "M0", "M1", "M2", "M3", "D0", "F1", "E3", "X0",
    "Q0", "K0", "W0", "U003", "D1", "E2", "F2", "U037", "P0", "X1", "K1", "D2",
    "W1", "U104", "F3", "B0", "U147", "X2", "P1", "D3", "K2", "W2", "R0", "U203",
    "B1", "U235", "X3", "U257", "S0", "P2", "R1", "K3", "W3", "U303", "B2", "U335",
    "S1", "U357", "R2", "P301", "P313", "B30", "P334", "S2", "B31", "R3", "S3",
)


def layer_kernel(names, chips, exp_count, capacity, *refs):
    v = types.SimpleNamespace(**dict(zip(names, refs)))
    seq, exp = lax.axis_index("seq"), lax.axis_index("exp")
    chip, core = seq // CORES, lax.rem(seq, CORES)
    other = 1 - core
    tok_rows, width = v.queries.shape
    head_lanes = HEAD_WIDTH
    half = width // CORES
    both_rows = CORES * tok_rows
    rows = CORES * capacity
    depth = exp_count * width
    blocks = v.first_mat.shape[0]
    block = v.first_mat.shape[2] // 2
    inside = (chip > 0) & (chip < chips - 1)
    source_of = [flip(chip, i) for i in range(chips)]
    first = flip(exp, 1) * other + flip(exp, 2) * core
    second = flip(exp, 2) * other + flip(exp, 1) * core
    diag = flip(exp, 3)
    j_first, j_second = 1 + core, 2 - core
    at = lambda c, e=exp: {"seq": chip * CORES + c, "exp": e}
    partner = at(other)
    sent = []

    def aligned(value, size, step):
        return pl.ds(pl.multiple_of(value, step), size)

    def send(src, dst, send_sem, recv_sem, target):
        c = remote(src, dst, send_sem, recv_sem, target)
        c.start()
        sent.append(c)
        return c

    def arrived(dst, send_sem, recv_sem):
        remote(dst, dst, send_sem, recv_sem, partner).wait_recv()

    small = [
        pltpu.make_async_copy(getattr(v, a), getattr(v, b), v.load_sem.at[i])
        for i, (a, b) in enumerate(
            (("keys", "k_in"), ("values", "v_in"), ("queries", "q_in"), ("residual", "r_in"))
        )
    ]
    for c in small:
        c.start()

    raw = v.raw
    raw[...] = jnp.full(raw.shape, -1.0, F32)
    raw[0:TOP, 0:tok_rows] = v.routes[...].astype(F32)
    raw[TOP : 2 * TOP, 0:tok_rows] = v.gates[...]
    table = raw[...]
    named = lax.broadcasted_iota(jnp.int32, table.shape, 0).astype(F32)
    one = [jnp.where(named == table[k : k + 1, :], 1.0, 0.0) for k in range(TOP)]
    lanes = (LANES, LANES)
    earlier = jnp.where(
        lax.broadcasted_iota(jnp.int32, lanes, 0) < lax.broadcasted_iota(jnp.int32, lanes, 1), 1.0, 0.0
    )
    before = jnp.dot(sum(one).astype(BF16), earlier.astype(BF16), preferred_element_type=F32)
    meta = v.meta
    meta[...] = table
    for k in range(TOP):
        meta[k : k + 1, :] = table[k : k + 1, :] * capacity + jnp.sum(
            one[k] * before, axis=0, keepdims=True
        )
    v.k_all[...] = jnp.zeros(v.k_all.shape, BF16)
    v.v_all[...] = jnp.zeros(v.v_all.shape, BF16)

    barrier = pltpu.get_barrier_semaphore()
    peers = [partner]
    for d in range(1, chips):
        for h in range(CORES):
            peers.append({"seq": lax.rem(chip + d, chips) * CORES + h, "exp": exp})
    for d in range(1, exp_count):
        for h in range(CORES):
            peers.append({"seq": chip * CORES + h, "exp": flip(exp, d)})
    for target in peers:
        pl.semaphore_signal(barrier, inc=1, device_id=target, device_id_type=pl.DeviceIdType.MESH)
    pl.semaphore_wait(barrier, len(peers))

    own_rows = aligned(seq * tok_rows, tok_rows, tok_rows)
    small[0].wait()
    small[1].wait()
    pairs = (("k_in", "k_all"), ("v_in", "v_all"))
    kv_send, kv_recv = v.kv_send, v.kv_recv
    for d in range(chips - 1, 0, -1):

        @pl.when(chip + d < chips)
        def _():
            for i, (a, b) in enumerate(pairs):
                for h in range(CORES):
                    remote(
                        getattr(v, a).at[:, h * head_lanes : (h + 1) * head_lanes],
                        getattr(v, b).at[own_rows, :],
                        kv_send.at[i, d, h],
                        kv_recv.at[i, d, core],
                        {"seq": (chip + d) * CORES + h, "exp": exp},
                    ).start()

    for i, (a, b) in enumerate(pairs):
        send(
            getattr(v, a).at[:, aligned(other * head_lanes, head_lanes, head_lanes)],
            getattr(v, b).at[own_rows, :],
            kv_send.at[i, 0, 0],
            kv_recv.at[i, 0, core],
            partner,
        )
    mine_rows = aligned(core * tok_rows, tok_rows, tok_rows)
    other_rows = aligned(other * tok_rows, tok_rows, tok_rows)
    mine_lanes = aligned(core * half, half, half)
    other_lanes = aligned(other * half, half, half)
    small[2].wait()
    small[3].wait()
    for i, (a, b) in enumerate((("q_in", "q_half"), ("r_in", "r_half"))):
        send(
            getattr(v, a).at[:, other_lanes],
            getattr(v, b).at[mine_rows, :],
            v.pair_send.at[i],
            v.pair_recv.at[i],
            partner,
        )
    for d in range(chips):
        for h in range(CORES):
            if d:
                target = {"seq": lax.rem(chip + d, chips) * CORES + h, "exp": exp}
            elif h == 0:
                target = partner
            else:
                continue
            send(meta, v.meta_all.at[seq], v.meta_send.at[d, h], v.meta_recv.at[d, core], target)
    loads = []
    for i in range(blocks):
        for m, a in enumerate(("w_gate", "w_up")):
            loads.append(
                pltpu.make_async_copy(
                    getattr(v, a).at[:, i * block : (i + 1) * block],
                    v.first_mat.at[i, :, m * block : (m + 1) * block],
                    v.gate_sem.at[m, i],
                )
            )
    for j in range(exp_count):
        loads.append(
            pltpu.make_async_copy(
                v.w_down.at[:, j * width : (j + 1) * width], v.down_mat.at[j], v.down_sem.at[j]
            )
        )
    for c in loads:
        c.start()
    v.meta_all[seq] = meta[...]
    for a, b in pairs:
        getattr(v, b)[own_rows, :] = getattr(v, a)[:, aligned(core * head_lanes, head_lanes, head_lanes)]
    for a, b in (("q_in", "q_half"), ("r_in", "r_half")):
        getattr(v, b)[mine_rows, :] = getattr(v, a)[:, mine_lanes]

    for i, b in enumerate(("q_half", "r_half")):
        arrived(getattr(v, b).at[other_rows, :], v.pair_send.at[i], v.pair_recv.at[i])
    for i, (a, b) in enumerate(pairs):
        there = aligned((chip * CORES + other) * tok_rows, tok_rows, tok_rows)
        arrived(getattr(v, b).at[there, :], kv_send.at[i, 0, 0], kv_recv.at[i, 0, other])
    for d in range(1, chips):

        @pl.when(chip - d >= 0)
        def _():
            for i, (a, b) in enumerate(pairs):
                for h in range(CORES):
                    there = aligned(((chip - d) * CORES + h) * tok_rows, tok_rows, tok_rows)
                    arrived(getattr(v, b).at[there, :], kv_send.at[i, d, h], kv_recv.at[i, d, h])

    length = v.k_all.shape[0]
    score_scale = 1.0 / math.sqrt(HEAD_WIDTH)
    shape = (both_rows, length)
    reach = lax.broadcasted_iota(jnp.int32, shape, 0) + chip * both_rows
    mask = lax.broadcasted_iota(jnp.int32, shape, 1) <= reach
    att = v.att
    square = jnp.zeros((both_rows, 1), F32)
    for i in range(half // HEAD_WIDTH):
        part = slice(i * HEAD_WIDTH, (i + 1) * HEAD_WIDTH)
        scores = (
            lax.dot_general(
                v.q_half[:, part], v.k_all[...], (((1,), (1,)), ((), ())),
                preferred_element_type=F32,
            )
            * score_scale
        )
        scores = jnp.where(mask, scores, -1e30)
        terms = jnp.where(mask, jnp.exp(scores - jnp.max(scores, axis=1, keepdims=True)), 0.0)
        weighted = jnp.dot(terms.astype(BF16), v.v_all[...], preferred_element_type=F32)
        value = weighted / jnp.sum(terms, axis=1, keepdims=True)
        value = (v.r_half[:, part].astype(F32) + value).astype(BF16)
        att[:, part] = value
        value = value.astype(F32)
        square = square + jnp.sum(value * value, axis=1, keepdims=True)
    block_eye = lax.broadcasted_iota(jnp.int32, (tok_rows, LANES), 0) == lax.broadcasted_iota(
        jnp.int32, (tok_rows, LANES), 1
    )
    squares, scales = v.squares, v.scales
    tokens, near, x_full, peer = v.tokens, v.near, v.x_full, v.peer
    tokens[chip] = (att[...].astype(F32) * v.gain[:, mine_lanes]).astype(BF16)

    def ship(source, wait):
        for way, test, to in ((0, (source <= chip) & (chip + 1 < chips), 1), (1, (source >= chip) & (chip > 0), -1)):

            @pl.when(test)
            def _():
                c = remote(
                    tokens.at[source], tokens.at[source],
                    v.far_send.at[source, way], v.far_recv.at[source],
                    {"seq": (chip + to) * CORES + core, "exp": exp},
                )
                if wait:
                    c.wait_send()
                else:
                    c.start()

    def landed(source):
        arrived(tokens.at[source], v.far_send.at[source, 0], v.far_recv.at[source])

    ship(chip, False)

    def deliver(which, ref):
        send(
            ref.at[other_rows, :], v.theirs.at[which],
            v.pair_send.at[2 + which], v.pair_recv.at[2 + which], partner,
        )
        c = pltpu.make_async_copy(
            ref.at[mine_rows, :], v.ours.at[which], v.store_sem.at[which]
        )
        c.start()
        stores.append(c)

    stores = []

    def spread():
        for b in range(CORES):
            squares[core, exp, b : b + 1, :] = jnp.sum(
                jnp.where(block_eye, square[b * tok_rows : (b + 1) * tok_rows], 0.0), axis=0, keepdims=True
            )
        for d in range(exp_count):
            for h in range(CORES):
                if d:
                    target = at(h, flip(exp, d))
                elif h == 0:
                    target = partner
                else:
                    continue
                send(
                    squares.at[core, exp], squares.at[core, exp],
                    v.square_send.at[d, h], v.square_recv.at[d, core], target,
                )
        deliver(0, att)
        for d in range(chips):
            for h in range(CORES):
                source = lax.rem(chip - d + chips, chips)
                if d:
                    arrived(
                        v.meta_all.at[source * CORES + h], v.meta_send.at[d, h], v.meta_recv.at[d, h]
                    )
                elif h == 0:
                    arrived(
                        v.meta_all.at[chip * CORES + other],
                        v.meta_send.at[0, 0], v.meta_recv.at[0, other],
                    )

    def stage_q(i):
        arrived(squares.at[other, exp], v.square_send.at[0, 0], v.square_recv.at[0, other])
        for d in range(1, exp_count):
            for h in range(CORES):
                arrived(squares.at[h, flip(exp, d)], v.square_send.at[d, h], v.square_recv.at[d, h])
        total = jnp.zeros(squares.shape[2:], F32)
        for e in range(exp_count):
            for h in range(CORES):
                total = total + squares[h, e]
        scales[chip] = lax.rsqrt(total / depth + 1e-05)
        for d in range(1, chips):
            send(
                scales.at[chip], scales.at[chip], v.scale_send.at[d], v.scale_recv.at[d],
                {"seq": lax.rem(chip + d, chips) * CORES + core, "exp": exp},
            )

    on_first, on_second = at(core, first), at(core, second)
    pair_of = {}

    def lane_of(slice_at, c):
        return aligned(slice_at * width + c * half, half, half)

    def give(turn, piece, slice_at):
        place = x_full.at[turn, :, lane_of(slice_at, core)]
        pair_of[turn, piece] = send(
            place, place, v.give_send.at[turn, piece], v.give_recv.at[turn, piece], partner
        )

    def tables(turn):
        iota = lax.broadcasted_iota(jnp.int32, (capacity, tok_rows), 0).astype(F32)
        hits, named = [], []
        for b in range(CORES):
            names_of = v.meta_all[source_of[turn] * CORES + b]
            dest = [names_of[k : k + 1, 0:tok_rows] for k in range(TOP)]
            hits.append([[iota == dest[k] - low[x] for k in range(TOP)] for x in range(2)])
            named.append(names_of)
        return hits, named

    low = [(e * capacity).astype(F32) for e in (exp, second)]

    def gathered(turn, value):
        out = [
            jnp.dot(
                v.picks[turn, b], value[b * tok_rows : (b + 1) * tok_rows, :], preferred_element_type=F32
            )
            for b in range(CORES)
        ]
        return [
            jnp.concatenate([o[x * capacity : (x + 1) * capacity] for o in out], axis=0).astype(BF16)
            for x in range(2)
        ]

    def stage_f(turn):
        source = source_of[turn]
        if turn == 1:
            landed(source)
            ship(source, False)
        elif turn:

            @pl.when(jnp.logical_not(inside))
            def _():
                landed(source)

        send(tokens.at[source], near.at[turn], v.near_send.at[turn], v.near_recv.at[turn], on_first)
        if turn == 0:
            spread()
            stage_t(turn)
        mine, away = gathered(turn, tokens[source])
        v.outbox[turn, 0] = away
        x_full[turn, :, lane_of(exp, core)] = mine
        push(turn, 0, exp)
        give(turn, 0, exp)

    def stage_t(turn):
        hits, _ = tables(turn)
        for b in range(CORES):
            v.picks[turn, b] = jnp.concatenate(
                [jnp.where(hits[b][x][0] | hits[b][x][1], 1.0, 0.0) for x in range(2)], axis=0
            ).astype(BF16)

    def stage_e(turn):
        @pl.when(inside)
        def _():
            landed(source_of[turn])
            ship(source_of[turn], False)

    def stage_d(turn):
        arrived(near.at[turn], v.near_send.at[turn], v.near_recv.at[turn])
        mine, away = gathered(turn, near[turn])
        v.outbox[turn, 1] = away
        x_full[turn, :, lane_of(first, core)] = mine
        push(turn, 1, first)
        give(turn, 1, first)

    def stage_k(turn):
        source = source_of[turn]
        if turn:
            for d in range(1, chips):

                @pl.when(lax.rem(chip - source + chips, chips) == d)
                def _():
                    arrived(scales.at[source], v.scale_send.at[d], v.scale_recv.at[d])

        hits, named = tables(turn)
        weights, norms = [], []
        for b in range(CORES):
            mine = hits[b][0]
            gate = [named[b][TOP + k : TOP + k + 1, 0:tok_rows] for k in range(TOP)]
            weights.append(
                sum(jnp.sum(jnp.where(mine[k], gate[k], 0.0), axis=1, keepdims=True) for k in range(TOP))
            )
            norm = scales[source, b : b + 1, 0:tok_rows]
            norms.append(
                sum(jnp.sum(jnp.where(mine[k], norm, 0.0), axis=1, keepdims=True) for k in range(TOP))
            )
        v.row_gate[turn] = jnp.broadcast_to(jnp.concatenate(weights, axis=0), (rows, LANES))
        v.row_norm[turn] = jnp.broadcast_to(jnp.concatenate(norms, axis=0), (rows, LANES))

    def stage_m(turn):
        place_of = lax.broadcasted_iota(jnp.int32, (tok_rows, rows), 1).astype(F32)
        for b in range(CORES):
            names_of = v.meta_all[source_of[turn] * CORES + b]
            columns = [
                jnp.sum(jnp.where(block_eye, names_of[k : k + 1, :], 0.0), axis=1, keepdims=True)
                for k in range(TOP)
            ]
            for x in range(2):
                mark = None
                for k in range(TOP):
                    column = columns[k] - low[x]
                    column = jnp.where(
                        (column >= 0.0) & (column < capacity), column + float(b * capacity), -1.0
                    )
                    hit = place_of == column
                    mark = hit if mark is None else mark | hit
                v.mixer[turn, x, b * tok_rows : (b + 1) * tok_rows, :] = jnp.where(mark, 1.0, 0.0).astype(BF16)

    def push(turn, piece, slice_at):
        send(
            v.outbox.at[turn, piece],
            x_full.at[turn, :, lane_of(slice_at, core)],
            v.push_send.at[turn, piece],
            v.push_recv.at[turn, piece],
            on_second,
        )

    def stage_x(turn):
        for piece, slice_at in ((0, second), (1, diag)):
            arrived(
                x_full.at[turn, :, lane_of(slice_at, core)],
                v.push_send.at[turn, piece],
                v.push_recv.at[turn, piece],
            )
            give(turn, 2 + piece, slice_at)

    def stage_w(turn):
        for piece, slice_at in enumerate((exp, second, first, diag)):
            arrived(
                x_full.at[turn, :, lane_of(slice_at, other)],
                v.give_send.at[turn, piece],
                v.give_recv.at[turn, piece],
            )

    def stage_u(turn, start, stop):
        start, stop = (blocks * start // 7, blocks * stop // 7)
        if turn == 0:
            for c in loads[2 * start : 2 * stop]:
                c.wait()

        def one(i, carry):
            out = jnp.dot(x_full[turn], v.first_mat[i], preferred_element_type=F32)
            norm = v.row_norm[turn, :, 0:1]
            gate = out[:, :block] * norm
            up = out[:, block:] * norm
            v.hidden[turn, :, aligned(i * block, block, block)] = (
                gate / (1.0 + jnp.exp(-gate)) * up
            ).astype(BF16)
            return carry

        lax.fori_loop(start, stop, one, 0)

    down_ready = []

    def stage_p(turn, start=0, stop=RANKS):
        if not down_ready:
            for c in loads[2 * blocks :]:
                c.wait()
            down_ready.append(True)
        for piece in range(4):
            if start:
                break
            c = pair_of[turn, piece]
            c.wait_send()
            sent[:] = [o for o in sent if o is not c]

        def one(step, carry):
            j = exp_count - 1 - step
            slice_at = exp + lax.rem(j, 2) * (1 - 2 * lax.rem(exp, 2)) + (j // 2) * (2 - 4 * (exp // 2))
            out = jnp.dot(v.hidden[turn], v.down_mat[slice_at], preferred_element_type=F32)
            x_full[turn, :, aligned(slice_at * width, width, width)] = out.astype(BF16)
            swap(turn, j, slice_at).start()
            return carry

        lax.fori_loop(start, stop, one, 0)
        for step in range(start, stop):
            j = exp_count - 1 - step
            sent.append(swap(turn, j, flip(exp, j)))

    def swap(turn, j, slice_at):
        return remote(
            x_full.at[turn, :, lane_of(slice_at, other)],
            peer.at[turn, j],
            v.peer_send.at[turn, j],
            v.peer_recv.at[turn, j],
            partner,
        )

    def stage_b(turn, part=None):
        weight = v.row_gate[turn, :, 0:1]
        last = exp_count - 1
        slices = {None: range(last, -1, -1), 0: [last], 1: range(last - 1, -1, -1)}[part]
        for j in slices:
            arrived(peer.at[turn, j], v.peer_send.at[turn, j], v.peer_recv.at[turn, j])
            total = x_full[turn, :, lane_of(flip(exp, j), core)].astype(F32) + peer[turn, j].astype(F32)
            peer[turn, j] = (total * weight).astype(BF16)
        pieces = ((1, last), (0, j_second))
        for piece, j in pieces if part is None else [pieces[part]]:
            send(
                peer.at[turn, j], v.back.at[turn, piece],
                v.back_send.at[turn, piece], v.back_recv.at[turn, piece], on_second,
            )

    def mixed(turn, j, piece):
        arrived(v.back.at[turn, piece], v.back_send.at[turn, piece], v.back_recv.at[turn, piece])
        return jnp.dot(v.mixer[turn, 0], peer[turn, j], preferred_element_type=F32) + jnp.dot(
            v.mixer[turn, 1], v.back[turn, piece], preferred_element_type=F32
        )

    def stage_r(turn):
        v.near_out[turn] = mixed(turn, j_first, 1).astype(BF16)
        send(
            v.near_out.at[turn], v.near_in.at[turn],
            v.home_send.at[turn], v.home_recv.at[turn], on_first,
        )

    def stage_s(turn):
        total = mixed(turn, 0, 0)
        arrived(v.near_in.at[turn], v.home_send.at[turn], v.home_recv.at[turn])
        total = total + v.near_in[turn].astype(F32)
        if turn == 0:
            v.total[...] = total + att[...].astype(F32)
        else:
            v.far_out[turn - 1] = total.astype(BF16)
            send(
                v.far_out.at[turn - 1], v.far_in.at[chip],
                v.last_send.at[turn], v.last_recv.at[chip],
                {"seq": source_of[turn] * CORES + core, "exp": exp},
            )

    stages = {
        "F": stage_f, "D": stage_d, "X": stage_x, "W": stage_w, "U": stage_u, "E": stage_e,
        "P": stage_p, "B": stage_b, "R": stage_r, "S": stage_s, "Q": stage_q, "K": stage_k, "M": stage_m, "T": stage_t,
    }
    for step in PLAN:
        stages[step[0]](*map(int, step[1:]))
    total = v.total[...]
    for turn in range(1, chips):
        source = source_of[turn]
        arrived(v.far_in.at[source], v.last_send.at[turn], v.last_recv.at[source])
        total = total + v.far_in[source].astype(F32)
    v.q_half[...] = total.astype(BF16)
    deliver(1, v.q_half)
    for i in range(2):
        stores[i].wait()
        arrived(v.theirs.at[i], v.pair_send.at[2 + i], v.pair_recv.at[2 + i])
    for turn in range(chips):
        ship(source_of[turn], True)
    for c in sent:
        c.wait_send()
    for d in range(chips - 1, 0, -1):

        @pl.when(chip + d < chips)
        def _():
            for i, (a, b) in enumerate(pairs):
                for h in range(CORES):
                    remote(
                        getattr(v, a).at[:, h * head_lanes : (h + 1) * head_lanes],
                        getattr(v, b).at[own_rows, :],
                        kv_send.at[i, d, h],
                        kv_recv.at[i, d, core],
                        {"seq": (chip + d) * CORES + h, "exp": exp},
                    ).wait_send()


def fused(queries, keys, values, residual, norm_gain, routes, gates, w_gate, w_up, w_down, capacity):
    tok_rows, width = queries.shape
    kv_width = keys.shape[1]
    exp_count, seq_count = lax.axis_size("exp"), lax.axis_size("seq")
    chips = seq_count // CORES
    depth, inner = w_gate.shape[1:]
    half, both_rows, rows = width // CORES, CORES * tok_rows, CORES * capacity
    block = 2 * LANES if inner % (2 * LANES) == 0 else inner
    blocks = inner // block
    dma = pltpu.SemaphoreType.DMA
    bf = lambda *shape: pltpu.VMEM(shape, BF16)
    f32 = lambda *shape: pltpu.VMEM(shape, F32)
    inputs = dict(
        gain=norm_gain.reshape(1, width), routes=routes.T, gates=gates.T,
        queries=queries, keys=keys, values=values, residual=residual,
        w_gate=w_gate[0], w_up=w_up[0], w_down=w_down[0],
    )
    scratch = dict(
        k_in=bf(tok_rows, kv_width), v_in=bf(tok_rows, kv_width),
        q_in=bf(tok_rows, width), r_in=bf(tok_rows, width),
        q_half=bf(both_rows, half), r_half=bf(both_rows, half),
        k_all=bf(seq_count * tok_rows, HEAD_WIDTH), v_all=bf(seq_count * tok_rows, HEAD_WIDTH),
        raw=f32(8, LANES), meta=f32(8, LANES), meta_all=f32(seq_count, 8, LANES),
        squares=f32(CORES, exp_count, 8, LANES), scales=f32(chips, 8, LANES),
        att=bf(both_rows, half), total=f32(both_rows, half),
        tokens=bf(chips, both_rows, half), near=bf(chips, both_rows, half),
        outbox=bf(chips, 2, rows, half), x_full=bf(chips, rows, depth),
        peer=bf(chips, exp_count, rows, half), back=bf(chips, 2, rows, half),
        near_out=bf(chips, both_rows, half), near_in=bf(chips, both_rows, half),
        far_out=bf(chips - 1, both_rows, half), far_in=bf(chips, both_rows, half),
        row_gate=f32(chips, rows, LANES), row_norm=f32(chips, rows, LANES),
        picks=bf(chips, CORES, rows, tok_rows), mixer=bf(chips, 2, both_rows, rows),
        hidden=bf(chips, rows, inner),
        first_mat=bf(blocks, depth, 2 * block),
        down_mat=bf(exp_count, inner, width),
        load_sem=dma((4,)), store_sem=dma((2,)), gate_sem=dma((2, blocks)), down_sem=dma((exp_count,)),
        kv_send=dma((2, chips, CORES)), kv_recv=dma((2, chips, CORES)),
        pair_send=dma((4,)), pair_recv=dma((4,)),
        meta_send=dma((chips, CORES)), meta_recv=dma((chips, CORES)),
        square_send=dma((exp_count, CORES)), square_recv=dma((exp_count, CORES)),
        far_send=dma((chips, 2)), far_recv=dma((chips,)),
        scale_send=dma((chips,)), scale_recv=dma((chips,)),
        near_send=dma((chips,)), near_recv=dma((chips,)),
        push_send=dma((chips, 2)), push_recv=dma((chips, 2)),
        give_send=dma((chips, 4)), give_recv=dma((chips, 4)),
        peer_send=dma((chips, exp_count)), peer_recv=dma((chips, exp_count)),
        back_send=dma((chips, 2)), back_recv=dma((chips, 2)),
        home_send=dma((chips,)), home_recv=dma((chips,)),
        last_send=dma((chips,)), last_recv=dma((chips,)),
    )
    vmem = pl.BlockSpec(memory_space=pltpu.VMEM)
    any_space = pl.BlockSpec(memory_space=pl.ANY)
    out = jax.ShapeDtypeStruct((2, tok_rows, half), BF16)
    names = list(inputs) + ["ours", "theirs"] + list(scratch)
    ours, theirs = pl.pallas_call(
        functools.partial(layer_kernel, names, chips, exp_count, capacity),
        out_shape=(out, out),
        in_specs=[vmem] * 3 + [any_space] * (len(inputs) - 3),
        out_specs=(any_space, any_space),
        scratch_shapes=list(scratch.values()),
        compiler_params=pltpu.CompilerParams(
            collective_id=1, has_side_effects=True, vmem_limit_bytes=67043328
        ),
    )(*inputs.values())
    left_is_ours = lax.rem(lax.axis_index("seq"), CORES) == 0
    both = jnp.concatenate(
        [jnp.where(left_is_ours, ours, theirs), jnp.where(left_is_ours, theirs, ours)], axis=2
    )
    return both[0], both[1]


def shards(queries, keys, values, residual, norm_gain, routes, gates, w_gate, w_up, w_down):
    tok_rows, local_width = queries.shape
    kv_width = keys.shape[1]
    local_heads = kv_width // HEAD_WIDTH
    group_width = QUERY_HEADS // KEY_VALUE_HEADS
    exp_count = lax.axis_size("exp")
    seq_count = lax.axis_size("seq")
    chips = seq_count // CORES
    dma = pltpu.SemaphoreType.DMA

    experts = exp_count * w_gate.shape[0]
    capacity = min(tok_rows, 3 * TOP * tok_rows // (2 * experts))
    group = 1
    while (group * capacity) % 16:
        group *= 2
    rows = group * capacity
    groups = chips // group
    if exp_count == 4 and chips == RANKS and local_heads == CORES and capacity % 8 == 0:
        return fused(
            queries, keys, values, residual, norm_gain, routes, gates, w_gate, w_up, w_down, capacity
        )

    raw = jnp.concatenate([routes.astype(F32), gates], axis=1).T
    raw = jnp.pad(
        raw, ((0, 8 - 2 * TOP), (0, LANES - tok_rows)), constant_values=-1.0
    )
    gain = norm_gain.reshape(1, local_width)

    k_all, v_all, meta_all, gain_all = call(
        functools.partial(share_kernel, chips, exp_count, capacity),
        (
            jax.ShapeDtypeStruct((seq_count, tok_rows, kv_width), BF16),
            jax.ShapeDtypeStruct((seq_count, tok_rows, kv_width), BF16),
            jax.ShapeDtypeStruct((chips, 8, LANES), F32),
            jax.ShapeDtypeStruct((exp_count, 1, local_width), F32),
        ),
        [
            pltpu.VMEM((8, LANES), F32),
            dma((3, chips)), dma((3, chips)), dma((2, chips)), dma((2, chips)),
            dma((exp_count,)), dma((exp_count,)), dma((4,)),
        ],
        1,
        keys, values, raw, gain,
    )

    score_scale = 1.0 / math.sqrt(HEAD_WIDTH)
    first_pos = lax.axis_index("seq") * tok_rows
    query_pos = first_pos + jnp.arange(tok_rows, dtype=jnp.int32)
    length = seq_count * tok_rows
    key_block = k_all.reshape(length, kv_width)
    value_block = v_all.reshape(length, kv_width)
    causal_mask = jnp.arange(length, dtype=jnp.int32)[None, :] <= query_pos[:, None]
    mask = jnp.concatenate([causal_mask] * group_width, axis=0)
    heads = []
    for h in range(local_heads):
        lanes = slice(h * HEAD_WIDTH, (h + 1) * HEAD_WIDTH)
        first = h * group_width * HEAD_WIDTH
        q = jnp.concatenate(
            [
                queries[:, first + i * HEAD_WIDTH : first + (i + 1) * HEAD_WIDTH]
                for i in range(group_width)
            ],
            axis=0,
        )
        scores = (
            lax.dot_general(
                q, key_block[:, lanes], (((1,), (1,)), ((), ())), preferred_element_type=F32
            )
            * score_scale
        )
        scores = jnp.where(mask, scores, -1e30)
        terms = jnp.where(mask, jnp.exp(scores - jnp.max(scores, axis=1, keepdims=True)), 0.0)
        weighted = jnp.dot(terms.astype(BF16), value_block[:, lanes], preferred_element_type=F32)
        out = weighted / jnp.sum(terms, axis=1, keepdims=True)
        heads += [out[i * tok_rows : (i + 1) * tok_rows] for i in range(group_width)]
    attn = jnp.concatenate(heads, axis=1)
    attended = (residual.astype(F32) + attn).astype(BF16)

    inner = w_gate.shape[2]
    block = 256 if inner % 256 == 0 else inner
    blocks = inner // block
    hidden = call(
        functools.partial(gather_kernel, chips, exp_count, group, capacity),
        jax.ShapeDtypeStruct((groups, blocks, CORES * rows, block), BF16),
        [
            pltpu.VMEM((groups, CORES, rows, exp_count * local_width), BF16),
            pltpu.VMEM((blocks, exp_count * local_width, block), BF16),
            pltpu.VMEM((blocks, exp_count * local_width, block), BF16),
            pltpu.VMEM((chips, tok_rows, local_width), BF16),
            pltpu.VMEM((groups, exp_count - 1, rows, local_width), BF16),
            pltpu.VMEM((groups, exp_count, rows, local_width), BF16),
            dma((chips,)), dma((chips,)),
            dma((groups, exp_count)), dma((groups, exp_count)),
            dma((groups,)), dma((groups,)),
            dma((2, blocks)),
        ],
        2,
        attended, meta_all, gain_all,
        streamed=(w_gate[0], w_up[0]),
    )
    meta_columns = jnp.swapaxes(meta_all, 1, 2)[:, :tok_rows, :]
    layer_out = call(
        functools.partial(return_kernel, chips, exp_count, group, capacity),
        jax.ShapeDtypeStruct((tok_rows, local_width), BF16),
        [
            pltpu.VMEM((exp_count, inner, local_width), BF16),
            pltpu.VMEM((groups, exp_count, CORES, rows, local_width), BF16),
            pltpu.VMEM((groups, exp_count, rows, local_width), BF16),
            pltpu.VMEM((groups, exp_count - 1, rows, local_width), BF16),
            pltpu.VMEM((groups, exp_count, rows, local_width), BF16),
            pltpu.VMEM((chips, tok_rows, local_width), BF16),
            pltpu.VMEM((chips, tok_rows, local_width), BF16),
            dma((chips,)), dma((chips,)),
            dma((groups, exp_count)), dma((groups, exp_count)),
            dma((groups, exp_count)), dma((groups, exp_count)),
            dma((exp_count,)),
        ],
        3,
        hidden, attended, meta_columns,
        streamed=(w_down[0],),
    )
    return (attended, layer_out)


def solution(mesh):
    in_specs = (
        P("seq", "exp"),
        P("seq", "exp"),
        P("seq", "exp"),
        P("seq", "exp"),
        P("exp"),
        P("seq", None),
        P("seq", None),
        P("exp", None, "seq"),
        P("exp", None, "seq"),
        P("exp", "seq", None),
    )
    out_specs = (P("seq", "exp"), P("seq", "exp"))
    return jax.shard_map(shards, mesh=mesh, in_specs=in_specs, out_specs=out_specs, check_vma=False)
```
